256 devices in a mesh: sec: 8 (over x, core), row: 32 (over z, y).
Axes of the slice: x: 4, y: 4, z: 8, core: 2. Of those that a mesh axis runs over, the one named last changes fastest.
Arguments:
- factor: float32 [8, 2048, 16384], P(None, 'row', 'sec'), may hold values from -0.046875 to 0.046875
- inverse_blocks: float32 [8, 2048, 2048], P('sec', 'row'), may hold values from -4 to 4, as said below
- right_side: float32 [8, 2048, 384], P('sec', 'row'), may hold values from -6 to 6
Outputs:
- solution: float32 [8, 2048, 384], P('sec', 'row')
The draws below stay inside these ranges and needn't reach their ends.
Inputs may be any that keep to these rules, and one draw needn't show every extreme that they name: `inverse_blocks`: each block is nonsingular; it stands for the inverse of the factor's diagonal block of that section.
All inputs are finite; a program needn't handle non-finite values.
Results may differ from the reference program's by a relative error of at most 0.0001.
Values sent between devices are 32-bit elements; how exact they have to be, the bound alone decides.
No kernel may reach another device: no remote copies, remote signals or barrier semaphores. Data moves between devices by JAX's collectives and lax.ppermute only.
A program may use at most 64 MiB of HBM per device.

```python
import math
import jax
import jax.numpy as jnp
from jax import lax

BLOCK = 2048
ORDER = 16384
COLS = 384
N_SEC = 8


def draw_inverse_blocks(key, part):
    first = jax.random.fold_in(jax.random.fold_in(key, 17), 0)
    noise = jnp.clip(jax.random.normal(first, (N_SEC, BLOCK, BLOCK), jnp.float32), -6.0, 6.0)
    blocks = jnp.eye(BLOCK, dtype=jnp.float32)[None] + 0.5 * noise / math.sqrt(BLOCK)
    return blocks


def steps_of(stream_key, shape, cuts, low, top_value):
    factor_of = 1.0
    for dim, parts in cuts:
        draws = jax.random.uniform(jax.random.fold_in(jax.random.fold_in(stream_key, 6), dim), (parts,), jnp.float32, low / len(cuts), top_value / len(cuts))
        factor_of = factor_of * jnp.repeat(jnp.exp(draws), shape[dim] // parts).reshape((-1,) + (1,) * (len(shape) - 1 - dim))
    return factor_of


def centred(stream_key, shape, spread, most, shards=(), kind=jnp.bfloat16):
    level = steps_of(stream_key, shape, shards, -0.22, 0.18) if shards else 1.0
    drawn = jax.random.normal(stream_key, shape, jnp.float32) * spread * level
    return jnp.minimum(jnp.maximum(drawn, -most), most).astype(kind)


def setup_inputs(seed: int = 0) -> dict:
    key_of = jax.random.split(jax.random.key(seed), 4)
    factor = centred(key_of[0], (N_SEC, BLOCK, ORDER), ORDER ** -0.5, 0.046875, ((1, 32), (2, 8)), jnp.float32)
    inverse_blocks = draw_inverse_blocks(jax.random.fold_in(key_of[3], 71), 0)
    right_side = centred(key_of[2], (N_SEC, BLOCK, COLS), 1.0, 6.0, ((0, 8), (1, 32)), jnp.float32)
    return dict(factor=factor, inverse_blocks=inverse_blocks, right_side=right_side)


def reference(factor, inverse_blocks, right_side):
    carried = jnp.zeros(right_side.shape, jnp.float32)
    pieces = []
    for index in range(N_SEC):
        residual = right_side[index] - carried[index]
        result = jnp.dot(inverse_blocks[index], residual, precision=lax.Precision.HIGHEST)
        pieces.append(result)
        if index + 1 < N_SEC:
            block = factor[index + 1:, :, index * BLOCK:(index + 1) * BLOCK]
            update = jnp.einsum("ias,sw->iaw", block, result, precision=lax.Precision.HIGHEST)
            carried = carried.at[index + 1:].add(update)
    return jnp.stack(pieces)
```

```python
import functools

import jax
import jax.numpy as jnp
from jax import lax
from jax.experimental import pallas as pl
from jax.experimental.pallas import tpu as pltpu
from jax.sharding import PartitionSpec as P

LANES = 128
VMEM = pl.BlockSpec(memory_space=pltpu.VMEM)
ANY = pl.BlockSpec(memory_space=pl.ANY)


def low_lanes(shape):
    return lax.broadcasted_iota(jnp.int32, shape, 1) < LANES // 2


def pack_kernel(rhs_ref, out_ref):
    groups, half, _ = out_ref.shape
    rows = rhs_ref[...]
    turned = jnp.concatenate([rows, rows], axis=0).T
    low = low_lanes((half, LANES))
    for group in range(groups):
        start = 2 * group * half
        top = turned[start : start + half]
        bottom = turned[start + half : start + 2 * half]
        out_ref[group] = jnp.where(low, top, bottom)


def unpack_kernel(packed_ref, out_ref):
    groups = packed_ref.shape[0]
    pieces = []
    for group in range(groups):
        tile = packed_ref[group]
        pieces += [tile, pltpu.roll(tile, LANES // 2, 1)]
    turned = jnp.concatenate(pieces, axis=0).T
    out_ref[...] = turned[: LANES // 2]


def split(values):
    high = values.astype(jnp.bfloat16)
    low = (values - high.astype(jnp.float32)).astype(jnp.bfloat16)
    return high, low


def spread(gathered_ref, whole_ref, parts_ref):
    devices, half, _ = gathered_ref.shape
    low = low_lanes((half, LANES))
    for pair in range(devices // 2):
        first = gathered_ref[2 * pair]
        second = gathered_ref[2 * pair + 1]
        lanes = slice(pair * LANES, (pair + 1) * LANES)
        whole_ref[:half, lanes] = jnp.where(low, first, pltpu.roll(second, LANES // 2, 1))
        whole_ref[half:, lanes] = jnp.where(low, pltpu.roll(first, LANES // 2, 1), second)
    high, rest = split(whole_ref[...])
    parts_ref[: 2 * half] = high
    parts_ref[2 * half :] = rest


def times(parts, matrix):
    cols = parts.shape[0] // 2
    high, low = split(matrix)
    dims = (((1,), (1,)), ((), ()))
    both = lax.dot_general(parts, high, dims, preferred_element_type=jnp.float32)
    rest = lax.dot_general(parts[:cols], low, dims, preferred_element_type=jnp.float32)
    return both[:cols] + (both[cols:] + rest)


def packed(turned):
    half = turned.shape[0] // 2
    return jnp.concatenate([turned[:half], turned[half:]], axis=1)


def apply_kernel(index, gathered_ref, matrix_ref, out_ref, block, whole, parts, sem):
    copy = pltpu.make_async_copy(matrix_ref.at[index], block, sem)
    copy.start()
    spread(gathered_ref, whole, parts)
    copy.wait()
    out_ref[...] = packed(times(parts[...], block[...]))


def residual_kernel(index, gathered_ref, base_ref, matrix_ref, out_ref, parts, block, whole, sem):
    copy = pltpu.make_async_copy(matrix_ref.at[index], block, sem)
    copy.start()
    spread(gathered_ref, whole, parts)
    copy.wait()
    out_ref[...] = base_ref[...] - packed(times(parts[...], block[...]))


def earlier_kernel(count, line, *refs):
    base_ref, matrix_ref = refs[:2]
    parts_refs = refs[2 : 2 + count]
    out_ref, blocks, sems = refs[2 + count :]
    copies = []
    for k in range(count):
        copy = pltpu.make_async_copy(matrix_ref.at[(k, line)], blocks.at[k], sems.at[k])
        copy.start()
        copies.append(copy)
    total = None
    for k in range(count):
        copies[k].wait()
        term = times(parts_refs[k][...], blocks[k])
        total = term if total is None else total + term
    out_ref[...] = base_ref[...] - packed(total)


def shards(factor, inverse_blocks, right_side):
    sections = lax.axis_size("sec")
    lines = lax.axis_size("row")
    local_rows, block = factor.shape[1:]
    cols = right_side.shape[2] // sections
    half = cols // 2
    tile = jax.ShapeDtypeStruct((half, LANES), jnp.float32)
    split_shape = (2 * cols, block)
    block_scratch = pltpu.VMEM((local_rows, block), jnp.float32)
    whole_scratch = pltpu.VMEM((cols, block), jnp.float32)
    parts_scratch = pltpu.VMEM(split_shape, jnp.bfloat16)

    inverses = lax.all_gather(inverse_blocks[0], "sec", axis=0)
    rows_of = {}
    for first, last in ((1, 2), (2, 4), (4, 6), (6, 8)):
        panel = lax.all_gather(factor[first:last], "sec", axis=0)
        for j in range(first, min(last, sections)):
            rows_of[j] = (panel, j - first)

    def exchange(shard):
        copies = jnp.broadcast_to(shard[None], (lines, *shard.shape))
        return lax.all_to_all(copies, "row", 0, 0, tiled=True)

    def apply(i, gathered):
        return pl.pallas_call(
            functools.partial(apply_kernel, (i,)),
            out_shape=tile,
            in_specs=[VMEM, ANY],
            out_specs=VMEM,
            scratch_shapes=[block_scratch, whole_scratch, parts_scratch, pltpu.SemaphoreType.DMA],
            name=f"apply_{i}",
        )(gathered, inverses)

    def residual(j, gathered, base):
        panel, line = rows_of[j]
        return pl.pallas_call(
            functools.partial(residual_kernel, (j - 1, line)),
            out_shape=(tile, jax.ShapeDtypeStruct(split_shape, jnp.bfloat16)),
            in_specs=[VMEM, VMEM, ANY],
            out_specs=(VMEM, VMEM),
            scratch_shapes=[block_scratch, whole_scratch, pltpu.SemaphoreType.DMA],
            name=f"residual_{j}",
        )(gathered, base, panel)

    def earlier(j, base, known):
        panel, line = rows_of[j]
        count = len(known)
        return pl.pallas_call(
            functools.partial(earlier_kernel, count, line),
            out_shape=tile,
            in_specs=[VMEM, ANY] + [VMEM] * count,
            out_specs=VMEM,
            scratch_shapes=[
                pltpu.VMEM((count, local_rows, block), jnp.float32),
                pltpu.SemaphoreType.DMA((count,)),
            ],
            name=f"earlier_{j}",
        )(base, panel, *known)

    chunks = pl.pallas_call(
        pack_kernel,
        out_shape=jax.ShapeDtypeStruct((sections, half, LANES), jnp.float32),
        in_specs=[VMEM],
        out_specs=VMEM,
        name="pack",
    )(right_side[0])
    given = lax.all_to_all(chunks, "sec", 0, 0, tiled=True)

    pieces = []
    known = []
    rest = given[0]
    for i in range(sections):
        gathered = exchange(rest)
        piece = apply(i, gathered)
        pieces.append(piece)
        if i + 1 < sections:
            base = given[i + 1]
            gathered = exchange(piece)
            if known:
                base = earlier(i + 1, base, known)
            rest, parts = residual(i + 1, gathered, base)
            known.append(parts)

    found = lax.all_to_all(jnp.stack(pieces), "sec", 0, 0, tiled=True)
    out = pl.pallas_call(
        unpack_kernel,
        out_shape=jax.ShapeDtypeStruct(right_side.shape[1:], jnp.float32),
        in_specs=[VMEM],
        out_specs=VMEM,
        name="unpack",
    )(found)
    return out[None]


def solution(mesh):
    return jax.shard_map(
        shards,
        mesh=mesh,
        in_specs=(P(None, "row", "sec"), P("sec", "row", None), P("sec", "row", None)),
        out_specs=P("sec", "row", None),
        check_vma=False,
    )
```

```python
import functools

import jax
import jax.numpy as jnp
from jax import lax
from jax.experimental import pallas as pl
from jax.experimental.pallas import tpu as pltpu
from jax.sharding import PartitionSpec as P

LANES = 128
VMEM = pl.BlockSpec(memory_space=pltpu.VMEM)
HBM = pl.BlockSpec(memory_space=pltpu.HBM)


def low_lanes(shape):
    return lax.broadcasted_iota(jnp.int32, shape, 1) < LANES // 2


def pack_kernel(rhs_ref, out_ref):
    groups, half, _ = out_ref.shape
    rows = rhs_ref[...]
    turned = jnp.concatenate([rows, rows], axis=0).T
    low = low_lanes((half, LANES))
    for group in range(groups):
        start = 2 * group * half
        top = turned[start : start + half]
        bottom = turned[start + half : start + 2 * half]
        out_ref[group] = jnp.where(low, top, bottom)


def unpack_kernel(packed_ref, out_ref):
    groups = packed_ref.shape[0]
    pieces = []
    for group in range(groups):
        tile = packed_ref[group]
        pieces += [tile, pltpu.roll(tile, LANES // 2, 1)]
    turned = jnp.concatenate(pieces, axis=0).T
    out_ref[...] = turned[: LANES // 2]


def split(values):
    high = values.astype(jnp.bfloat16)
    low = (values - high.astype(jnp.float32)).astype(jnp.bfloat16)
    return high, low


def spread(gathered_ref, whole_ref, parts_ref):
    devices, half, _ = gathered_ref.shape
    low = low_lanes((half, LANES))
    for pair in range(devices // 2):
        first = gathered_ref[2 * pair]
        second = gathered_ref[2 * pair + 1]
        lanes = slice(pair * LANES, (pair + 1) * LANES)
        whole_ref[:half, lanes] = jnp.where(low, first, pltpu.roll(second, LANES // 2, 1))
        whole_ref[half:, lanes] = jnp.where(low, pltpu.roll(first, LANES // 2, 1), second)
    high, rest = split(whole_ref[...])
    parts_ref[: 2 * half] = high
    parts_ref[2 * half :] = rest


def times(parts, matrix):
    cols = parts.shape[0] // 2
    high, low = split(matrix)
    dims = (((1,), (1,)), ((), ()))
    both = lax.dot_general(parts, high, dims, preferred_element_type=jnp.float32)
    rest = lax.dot_general(parts[:cols], low, dims, preferred_element_type=jnp.float32)
    return both[:cols] + (both[cols:] + rest)


def packed(turned):
    half = turned.shape[0] // 2
    return jnp.concatenate([turned[:half], turned[half:]], axis=1)


def fetch_kernel(index, matrix_ref, out_ref, sem):
    copy = pltpu.make_async_copy(matrix_ref.at[index], out_ref, sem)
    copy.start()
    copy.wait()


def apply_kernel(gathered_ref, matrix_ref, tile_ref, copies_ref, whole, parts):
    spread(gathered_ref, whole, parts)
    tile = packed(times(parts[...], matrix_ref[...]))
    tile_ref[...] = tile
    copies_ref[...] = jnp.broadcast_to(tile[None], copies_ref.shape)


def last_kernel(gathered_ref, matrix_ref, tile_ref, whole, parts):
    spread(gathered_ref, whole, parts)
    tile_ref[...] = packed(times(parts[...], matrix_ref[...]))


def residual_kernel(gathered_ref, base_ref, matrix_ref, copies_ref, parts, whole):
    spread(gathered_ref, whole, parts)
    tile = base_ref[...] - packed(times(parts[...], matrix_ref[...]))
    copies_ref[...] = jnp.broadcast_to(tile[None], copies_ref.shape)


def earlier_kernel(places, follow, *refs):
    count = len(places)
    base_ref, inverses_ref = refs[:2]
    panels = refs[2 : 2 + len(follow[1])]
    parts_refs = refs[2 + len(panels) : 2 + len(panels) + count - 1]
    base_out, matrix_out, inverse_out, blocks, sems = refs[2 + len(panels) + count - 1 :]
    targets = [blocks.at[k] for k in range(count - 1)] + [matrix_out]
    copies = []
    for k, (panel, slot) in enumerate(places):
        copies.append(pltpu.make_async_copy(panels[panel].at[slot], targets[k], sems.at[k]))
    copies.append(pltpu.make_async_copy(inverses_ref.at[follow[0]], inverse_out, sems.at[count]))
    for copy in copies:
        copy.start()
    total = base_ref[...]
    for k in range(count - 1):
        copies[k].wait()
        total = total - packed(times(parts_refs[k][...], blocks[k]))
    base_out[...] = total
    copies[count - 1].wait()
    copies[count].wait()


def in_vmem(value):
    return pltpu.with_memory_space_constraint(value, pltpu.VMEM)


def in_hbm(value):
    return pltpu.with_memory_space_constraint(value, pltpu.HBM)


def shards(factor, inverse_blocks, right_side):
    sections = lax.axis_size("sec")
    segment = lax.axis_index("sec")
    lines = lax.axis_size("row")
    local_rows, block = factor.shape[1:]
    cols = right_side.shape[2] // sections
    half = cols // 2
    f32 = jnp.float32
    tile = jax.ShapeDtypeStruct((half, LANES), f32)
    tile_in_vmem = pltpu.VMEM((half, LANES), f32)
    copies_in_vmem = pltpu.VMEM((lines, half, LANES), f32)
    parts_in_vmem = pltpu.VMEM((2 * cols, block), jnp.bfloat16)
    matrix_in_vmem = pltpu.VMEM((local_rows, block), f32)
    whole_scratch = pltpu.VMEM((cols, block), f32)
    params = pltpu.CompilerParams(vmem_limit_bytes=24 << 20)

    chunks = pl.pallas_call(
        pack_kernel,
        out_shape=jax.ShapeDtypeStruct((sections, half, LANES), f32),
        in_specs=[VMEM],
        out_specs=VMEM,
        compiler_params=params,
        name="pack",
    )(right_side[0])
    given = lax.all_to_all(chunks, "sec", 0, 0, tiled=True)

    inverses = lax.all_gather(inverse_blocks[0], "sec", axis=0)

    middle = sections // 2

    def panel(factor, d):
        far = {1: sections, middle: sections - 1}.get(d, sections - d)
        own = lax.dynamic_index_in_dim(factor, jnp.minimum(segment + d, sections - 1), 0, False)
        if far < sections:
            sent = lax.dynamic_index_in_dim(
                factor, jnp.minimum(segment + far, sections - 1), 0, False
            )
            route = [(k, k + far) for k in range(sections - far)]
            moved = lax.ppermute(sent, "sec", route)
            own = jnp.where(segment + d < sections, own, moved)
        return lax.all_gather(own, "sec", axis=0)

    def place(j, k):
        d = j - k
        if d <= middle:
            return d, k
        return (middle if d + 1 == sections else sections - d), j

    panels = {1: panel(factor, 1)}

    def exchange(copies):
        return lax.all_to_all(copies, "row", 0, 0, tiled=True)

    def fetch(i):
        return pl.pallas_call(
            functools.partial(fetch_kernel, i),
            out_shape=matrix_in_vmem,
            in_specs=[HBM],
            out_specs=VMEM,
            scratch_shapes=[pltpu.SemaphoreType.DMA],
            compiler_params=params,
            name=f"fetch_{i}",
        )(in_hbm(inverses))

    def apply(i, gathered, inverse):
        last = i + 1 == sections
        return pl.pallas_call(
            last_kernel if last else apply_kernel,
            out_shape=tile if last else (tile, copies_in_vmem),
            in_specs=[VMEM, VMEM],
            out_specs=VMEM if last else (VMEM, VMEM),
            scratch_shapes=[whole_scratch, parts_in_vmem],
            compiler_params=params,
            name=f"apply_{i}",
        )(in_vmem(gathered), in_vmem(inverse))

    def residual(j, gathered, base, matrix):
        return pl.pallas_call(
            residual_kernel,
            out_shape=(copies_in_vmem, parts_in_vmem),
            in_specs=[VMEM, VMEM, VMEM],
            out_specs=(VMEM, VMEM),
            scratch_shapes=[whole_scratch],
            compiler_params=params,
            name=f"residual_{j}",
        )(in_vmem(gathered), in_vmem(base), in_vmem(matrix))

    def earlier(j, base, known):
        where = [place(j, k) for k in range(j)]
        used = sorted({d for d, _ in where})
        places = [(used.index(d), slot) for d, slot in where]
        return pl.pallas_call(
            functools.partial(earlier_kernel, places, (j, used)),
            out_shape=(tile_in_vmem, matrix_in_vmem, matrix_in_vmem),
            in_specs=[VMEM, HBM] + [HBM] * len(used) + [VMEM] * len(known),
            out_specs=(VMEM, VMEM, VMEM),
            scratch_shapes=[
                pltpu.VMEM((max(j - 1, 1), local_rows, block), f32),
                pltpu.SemaphoreType.DMA((j + 1,)),
            ],
            compiler_params=params,
            name=f"earlier_{j}",
        )(
            base,
            in_hbm(inverses),
            *[in_hbm(panels[d]) for d in used],
            *[in_vmem(parts) for parts in known],
        )

    pieces = []
    known = []
    copies = jnp.broadcast_to(given[0][None], (lines, half, LANES))
    inverse = fetch(0)
    for i in range(sections):
        gathered = exchange(copies)
        if i == 0:
            gathered, factor = lax.optimization_barrier((gathered, factor))
            panels |= {d: panel(factor, d) for d in range(2, middle + 1)}
        if i + 1 == sections:
            pieces.append(apply(i, gathered, inverse))
            break
        piece, copies = apply(i, gathered, inverse)
        pieces.append(piece)
        gathered = exchange(copies)
        base, matrix, inverse = earlier(i + 1, given[i + 1], known)
        copies, parts = residual(i + 1, gathered, base, matrix)
        known.append(parts)

    found = lax.all_to_all(jnp.stack(pieces), "sec", 0, 0, tiled=True)
    out = pl.pallas_call(
        unpack_kernel,
        out_shape=jax.ShapeDtypeStruct(right_side.shape[1:], f32),
        in_specs=[VMEM],
        out_specs=VMEM,
        compiler_params=params,
        name="unpack",
    )(found)
    return out[None]


def solution(mesh):
    return jax.shard_map(
        shards,
        mesh=mesh,
        in_specs=(P(None, "row", "sec"), P("sec", "row", None), P("sec", "row", None)),
        out_specs=P("sec", "row", None),
        check_vma=False,
    )
```

```python
import functools

import jax
import jax.numpy as jnp
from jax import lax
from jax.experimental import pallas as pl
from jax.experimental.pallas import tpu as pltpu
from jax.sharding import PartitionSpec as P

LANES = 128
VMEM = pl.BlockSpec(memory_space=pltpu.VMEM)
HBM = pl.BlockSpec(memory_space=pltpu.HBM)


def low_lanes(shape):
    return lax.broadcasted_iota(jnp.int32, shape, 1) < LANES // 2


def pack_kernel(rhs_ref, out_ref):
    groups, half, _ = out_ref.shape
    rows = rhs_ref[...]
    turned = jnp.concatenate([rows, rows], axis=0).T
    low = low_lanes((half, LANES))
    for group in range(groups):
        start = 2 * group * half
        top = turned[start : start + half]
        bottom = turned[start + half : start + 2 * half]
        out_ref[group] = jnp.where(low, top, bottom)


def unpack_kernel(packed_ref, out_ref):
    groups = packed_ref.shape[0]
    pieces = []
    for group in range(groups):
        tile = packed_ref[group]
        pieces += [tile, pltpu.roll(tile, LANES // 2, 1)]
    turned = jnp.concatenate(pieces, axis=0).T
    out_ref[...] = turned[: LANES // 2]


def split(values):
    high = values.astype(jnp.bfloat16)
    low = (values - high.astype(jnp.float32)).astype(jnp.bfloat16)
    return high, low


def spread(gathered_ref, whole_ref, parts_ref):
    devices, half, _ = gathered_ref.shape
    low = low_lanes((half, LANES))
    for pair in range(devices // 2):
        first = gathered_ref[2 * pair]
        second = gathered_ref[2 * pair + 1]
        lanes = slice(pair * LANES, (pair + 1) * LANES)
        whole_ref[:half, lanes] = jnp.where(low, first, pltpu.roll(second, LANES // 2, 1))
        whole_ref[half:, lanes] = jnp.where(low, pltpu.roll(first, LANES // 2, 1), second)
    high, rest = split(whole_ref[...])
    parts_ref[: 2 * half] = high
    parts_ref[2 * half :] = rest


def times(parts, matrix):
    cols = parts.shape[0] // 2
    high, low = split(matrix)
    dims = (((1,), (1,)), ((), ()))
    both = lax.dot_general(parts, high, dims, preferred_element_type=jnp.float32)
    rest = lax.dot_general(parts[:cols], low, dims, preferred_element_type=jnp.float32)
    return both[:cols] + (both[cols:] + rest)


def packed(turned):
    half = turned.shape[0] // 2
    return jnp.concatenate([turned[:half], turned[half:]], axis=1)


def fetch_kernel(index, matrix_ref, out_ref, sem):
    copy = pltpu.make_async_copy(matrix_ref.at[index], out_ref, sem)
    copy.start()
    copy.wait()


def apply_kernel(gathered_ref, matrix_ref, tile_ref, copies_ref, whole, parts):
    spread(gathered_ref, whole, parts)
    tile = packed(times(parts[...], matrix_ref[...]))
    tile_ref[...] = tile
    copies_ref[...] = jnp.broadcast_to(tile[None], copies_ref.shape)


def last_kernel(gathered_ref, matrix_ref, tile_ref, whole, parts):
    spread(gathered_ref, whole, parts)
    tile_ref[...] = packed(times(parts[...], matrix_ref[...]))


def residual_kernel(gathered_ref, base_ref, matrix_ref, copies_ref, parts, whole):
    spread(gathered_ref, whole, parts)
    tile = base_ref[...] - packed(times(parts[...], matrix_ref[...]))
    copies_ref[...] = jnp.broadcast_to(tile[None], copies_ref.shape)


def earlier_kernel(places, arrays, follow, *refs):
    count = len(places)
    base_ref = refs[0]
    panels = refs[1 : 1 + arrays]
    parts_refs = refs[1 + arrays : arrays + count]
    base_out, matrix_out, inverse_out, blocks, sems = refs[arrays + count :]
    targets = [blocks.at[k] for k in range(count - 1)] + [matrix_out]
    copies = []
    for k, (panel, slot) in enumerate(places):
        copies.append(pltpu.make_async_copy(panels[panel].at[slot], targets[k], sems.at[k]))
    copies.append(pltpu.make_async_copy(panels[0].at[follow], inverse_out, sems.at[count]))
    for copy in copies:
        copy.start()
    total = base_ref[...]
    for k in range(count - 1):
        copies[k].wait()
        total = total - packed(times(parts_refs[k][...], blocks[k]))
    base_out[...] = total
    copies[count - 1].wait()
    copies[count].wait()


def in_vmem(value):
    return pltpu.with_memory_space_constraint(value, pltpu.VMEM)


def in_hbm(value):
    return pltpu.with_memory_space_constraint(value, pltpu.HBM)


def shards(factor, inverse_blocks, right_side):
    sections = lax.axis_size("sec")
    segment = lax.axis_index("sec")
    lines = lax.axis_size("row")
    local_rows, block = factor.shape[1:]
    cols = right_side.shape[2] // sections
    half = cols // 2
    f32 = jnp.float32
    tile_in_vmem = pltpu.VMEM((half, LANES), f32)
    copies_in_vmem = pltpu.VMEM((lines, half, LANES), f32)
    parts_in_vmem = pltpu.VMEM((2 * cols, block), jnp.bfloat16)
    matrix_in_vmem = pltpu.VMEM((local_rows, block), f32)
    whole_scratch = pltpu.VMEM((cols, block), f32)
    params = pltpu.CompilerParams(vmem_limit_bytes=24 << 20)

    chunks = pl.pallas_call(
        pack_kernel,
        out_shape=jax.ShapeDtypeStruct((sections, half, LANES), f32),
        in_specs=[VMEM],
        out_specs=VMEM,
        compiler_params=params,
        name="pack",
    )(right_side[0])
    given = lax.all_to_all(chunks, "sec", 0, 0, tiled=True)

    def diagonal(d):
        return lax.dynamic_index_in_dim(factor, jnp.minimum(segment + d, sections - 1), 0, False)

    first = lax.all_gather(jnp.stack([inverse_blocks[0], diagonal(1)]), "sec", axis=0)
    panels = {1: (first, 1)}
    for group in ((2,), (3,), (4, 5), (6, 7)):
        gathered = lax.all_gather(jnp.stack([diagonal(d) for d in group]), "sec", axis=0)
        panels |= {d: (gathered, line) for line, d in enumerate(group)}

    def exchange(copies):
        return lax.all_to_all(copies, "row", 0, 0, tiled=True)

    def fetch(i):
        return pl.pallas_call(
            functools.partial(fetch_kernel, (i, 0)),
            out_shape=matrix_in_vmem,
            in_specs=[HBM],
            out_specs=VMEM,
            scratch_shapes=[pltpu.SemaphoreType.DMA],
            compiler_params=params,
            name=f"fetch_{i}",
        )(in_hbm(first))

    def apply(i, gathered, inverse):
        last = i + 1 == sections
        return pl.pallas_call(
            last_kernel if last else apply_kernel,
            out_shape=tile_in_vmem if last else (tile_in_vmem, copies_in_vmem),
            in_specs=[VMEM, VMEM],
            out_specs=VMEM if last else (VMEM, VMEM),
            scratch_shapes=[whole_scratch, parts_in_vmem],
            compiler_params=params,
            name=f"apply_{i}",
        )(in_vmem(gathered), in_vmem(inverse))

    def residual(j, gathered, base, matrix):
        return pl.pallas_call(
            residual_kernel,
            out_shape=(copies_in_vmem, parts_in_vmem),
            in_specs=[VMEM, VMEM, VMEM],
            out_specs=(VMEM, VMEM),
            scratch_shapes=[whole_scratch],
            compiler_params=params,
            name=f"residual_{j}",
        )(in_vmem(gathered), in_vmem(base), in_vmem(matrix))

    def earlier(j, base, known):
        arrays = [first]
        places = []
        for k in range(j):
            array, line = panels[j - k]
            if not any(array is other for other in arrays):
                arrays.append(array)
            index = [array is other for other in arrays].index(True)
            places.append((index, (k, line)))
        return pl.pallas_call(
            functools.partial(earlier_kernel, places, len(arrays), (j, 0)),
            out_shape=(tile_in_vmem, matrix_in_vmem, matrix_in_vmem),
            in_specs=[VMEM] + [HBM] * len(arrays) + [VMEM] * len(known),
            out_specs=(VMEM, VMEM, VMEM),
            scratch_shapes=[
                pltpu.VMEM((max(j - 1, 1), local_rows, block), f32),
                pltpu.SemaphoreType.DMA((j + 1,)),
            ],
            compiler_params=params,
            name=f"earlier_{j}",
        )(base, *[in_hbm(array) for array in arrays], *[in_vmem(parts) for parts in known])

    pieces = []
    known = []
    copies = jnp.broadcast_to(given[0][None], (lines, half, LANES))
    inverse = fetch(0)
    for i in range(sections):
        gathered = exchange(copies)
        if i + 1 == sections:
            pieces.append(apply(i, gathered, inverse))
            break
        piece, copies = apply(i, gathered, inverse)
        pieces.append(piece)
        gathered = exchange(copies)
        base, matrix, inverse = earlier(i + 1, given[i + 1], known)
        copies, parts = residual(i + 1, gathered, base, matrix)
        known.append(parts)

    found = lax.all_to_all(jnp.stack(pieces), "sec", 0, 0, tiled=True)
    out = pl.pallas_call(
        unpack_kernel,
        out_shape=jax.ShapeDtypeStruct(right_side.shape[1:], f32),
        in_specs=[VMEM],
        out_specs=VMEM,
        compiler_params=params,
        name="unpack",
    )(found)
    return out[None]


def solution(mesh):
    return jax.shard_map(
        shards,
        mesh=mesh,
        in_specs=(P(None, "row", "sec"), P("sec", "row", None), P("sec", "row", None)),
        out_specs=P("sec", "row", None),
        check_vma=False,
    )
```

```python
import functools

import jax
import jax.numpy as jnp
from jax import lax
from jax.experimental import pallas as pl
from jax.experimental.pallas import tpu as pltpu
from jax.sharding import PartitionSpec as P

LANES = 128
VMEM = pl.BlockSpec(memory_space=pltpu.VMEM)
HBM = pl.BlockSpec(memory_space=pltpu.HBM)


def low_lanes(shape):
    return lax.broadcasted_iota(jnp.int32, shape, 1) < LANES // 2


def pack_kernel(rhs_ref, out_ref):
    groups, half, _ = out_ref.shape
    rows = rhs_ref[...]
    turned = jnp.concatenate([rows, rows], axis=0).T
    low = low_lanes((half, LANES))
    for group in range(groups):
        start = 2 * group * half
        top = turned[start : start + half]
        bottom = turned[start + half : start + 2 * half]
        out_ref[group] = jnp.where(low, top, bottom)


def unpack_kernel(packed_ref, out_ref):
    groups = packed_ref.shape[0]
    pieces = []
    for group in range(groups):
        tile = packed_ref[group]
        pieces += [tile, pltpu.roll(tile, LANES // 2, 1)]
    turned = jnp.concatenate(pieces, axis=0).T
    out_ref[...] = turned[: LANES // 2]


def split(values):
    high = values.astype(jnp.bfloat16)
    low = (values - high.astype(jnp.float32)).astype(jnp.bfloat16)
    return high, low


def spread(gathered_ref, whole_ref, parts_ref):
    devices, half, _ = gathered_ref.shape
    low = low_lanes((half, LANES))
    for pair in range(devices // 2):
        first = gathered_ref[2 * pair]
        second = gathered_ref[2 * pair + 1]
        lanes = slice(pair * LANES, (pair + 1) * LANES)
        whole_ref[:half, lanes] = jnp.where(low, first, pltpu.roll(second, LANES // 2, 1))
        whole_ref[half:, lanes] = jnp.where(low, pltpu.roll(first, LANES // 2, 1), second)
    high, rest = split(whole_ref[...])
    parts_ref[: 2 * half] = high
    parts_ref[2 * half :] = rest


def times(parts, matrix):
    cols = parts.shape[0] // 2
    high, low = split(matrix)
    dims = (((1,), (1,)), ((), ()))
    both = lax.dot_general(parts, high, dims, preferred_element_type=jnp.float32)
    rest = lax.dot_general(parts[:cols], low, dims, preferred_element_type=jnp.float32)
    return both[:cols] + (both[cols:] + rest)


def packed(turned):
    half = turned.shape[0] // 2
    return jnp.concatenate([turned[:half], turned[half:]], axis=1)


def fetch_kernel(index, matrix_ref, out_ref, sem):
    copy = pltpu.make_async_copy(matrix_ref.at[index], out_ref, sem)
    copy.start()
    copy.wait()


def apply_kernel(gathered_ref, matrix_ref, tile_ref, copies_ref, whole, parts):
    spread(gathered_ref, whole, parts)
    tile = packed(times(parts[...], matrix_ref[...]))
    tile_ref[...] = tile
    copies_ref[...] = jnp.broadcast_to(tile[None], copies_ref.shape)


def last_kernel(gathered_ref, matrix_ref, *refs):
    earlier_refs = refs[:-3]
    out_ref, whole, parts = refs[-3:]
    for i, piece_ref in enumerate(earlier_refs):
        out_ref[i] = piece_ref[...]
    spread(gathered_ref, whole, parts)
    out_ref[len(earlier_refs)] = packed(times(parts[...], matrix_ref[...]))


def residual_kernel(gathered_ref, base_ref, matrix_ref, copies_ref, parts, whole):
    spread(gathered_ref, whole, parts)
    tile = base_ref[...] - packed(times(parts[...], matrix_ref[...]))
    copies_ref[...] = jnp.broadcast_to(tile[None], copies_ref.shape)


def earlier_kernel(places, arrays, follow, *refs):
    count = len(places)
    base_ref = refs[0]
    panels = refs[1 : 1 + arrays]
    parts_refs = refs[1 + arrays : arrays + count]
    base_out, matrix_out, inverse_out, blocks, sems = refs[arrays + count :]
    targets = [blocks.at[k] for k in range(count - 1)] + [matrix_out]
    copies = []
    for k, (panel, slot) in enumerate(places):
        copies.append(pltpu.make_async_copy(panels[panel].at[slot], targets[k], sems.at[k]))
    copies.append(pltpu.make_async_copy(panels[0].at[follow], inverse_out, sems.at[count]))
    for copy in copies:
        copy.start()
    total = base_ref[...]
    for k in range(count - 1):
        copies[k].wait()
        total = total - packed(times(parts_refs[k][...], blocks[k]))
    base_out[...] = total
    copies[count - 1].wait()
    copies[count].wait()


def in_vmem(value):
    return pltpu.with_memory_space_constraint(value, pltpu.VMEM)


def in_hbm(value):
    return pltpu.with_memory_space_constraint(value, pltpu.HBM)


def shards(factor, inverse_blocks, right_side):
    sections = lax.axis_size("sec")
    segment = lax.axis_index("sec")
    lines = lax.axis_size("row")
    local_rows, block = factor.shape[1:]
    cols = right_side.shape[2] // sections
    half = cols // 2
    f32 = jnp.float32
    tile_in_vmem = pltpu.VMEM((half, LANES), f32)
    copies_in_vmem = pltpu.VMEM((lines, half, LANES), f32)
    parts_in_vmem = pltpu.VMEM((2 * cols, block), jnp.bfloat16)
    matrix_in_vmem = pltpu.VMEM((local_rows, block), f32)
    whole_scratch = pltpu.VMEM((cols, block), f32)
    params = pltpu.CompilerParams(vmem_limit_bytes=24 << 20)

    chunks = pl.pallas_call(
        pack_kernel,
        out_shape=jax.ShapeDtypeStruct((sections, half, LANES), f32),
        in_specs=[VMEM],
        out_specs=VMEM,
        compiler_params=params,
        name="pack",
    )(right_side[0])
    given = lax.all_to_all(chunks, "sec", 0, 0, tiled=True)

    def panel(factor, d):
        own = lax.dynamic_index_in_dim(factor, jnp.minimum(segment + d, sections - 1), 0, False)
        return lax.all_gather(own, "sec", axis=0)

    inverses = lax.all_gather(inverse_blocks[0], "sec", axis=0)
    panels = {1: panel(factor, 1)}
    given, factor = lax.optimization_barrier((given, factor))
    panels |= {d: panel(factor, d) for d in range(2, sections)}

    def exchange(copies):
        return lax.all_to_all(copies, "row", 0, 0, tiled=True)

    def fetch(i):
        return pl.pallas_call(
            functools.partial(fetch_kernel, i),
            out_shape=matrix_in_vmem,
            in_specs=[HBM],
            out_specs=VMEM,
            scratch_shapes=[pltpu.SemaphoreType.DMA],
            compiler_params=params,
            name=f"fetch_{i}",
        )(in_hbm(inverses))

    def apply(i, gathered, inverse):
        return pl.pallas_call(
            apply_kernel,
            out_shape=(tile_in_vmem, copies_in_vmem),
            in_specs=[VMEM, VMEM],
            out_specs=(VMEM, VMEM),
            scratch_shapes=[whole_scratch, parts_in_vmem],
            compiler_params=params,
            name=f"apply_{i}",
        )(in_vmem(gathered), in_vmem(inverse))

    def apply_last(gathered, inverse, pieces):
        return pl.pallas_call(
            last_kernel,
            out_shape=pltpu.VMEM((sections, half, LANES), f32),
            in_specs=[VMEM, VMEM] + [VMEM] * len(pieces),
            out_specs=VMEM,
            scratch_shapes=[whole_scratch, parts_in_vmem],
            compiler_params=params,
            name="apply_last",
        )(in_vmem(gathered), in_vmem(inverse), *[in_vmem(piece) for piece in pieces])

    def residual(j, gathered, base, matrix):
        return pl.pallas_call(
            residual_kernel,
            out_shape=(copies_in_vmem, parts_in_vmem),
            in_specs=[VMEM, VMEM, VMEM],
            out_specs=(VMEM, VMEM),
            scratch_shapes=[whole_scratch],
            compiler_params=params,
            name=f"residual_{j}",
        )(in_vmem(gathered), in_vmem(base), in_vmem(matrix))

    def earlier(j, base, known):
        arrays = [inverses, *(panels[j - k] for k in range(j))]
        places = [(1 + k, k) for k in range(j)]
        return pl.pallas_call(
            functools.partial(earlier_kernel, places, len(arrays), j),
            out_shape=(tile_in_vmem, matrix_in_vmem, matrix_in_vmem),
            in_specs=[VMEM] + [HBM] * len(arrays) + [VMEM] * len(known),
            out_specs=(VMEM, VMEM, VMEM),
            scratch_shapes=[
                pltpu.VMEM((max(j - 1, 1), local_rows, block), f32),
                pltpu.SemaphoreType.DMA((j + 1,)),
            ],
            compiler_params=params,
            name=f"earlier_{j}",
        )(base, *[in_hbm(array) for array in arrays], *[in_vmem(parts) for parts in known])

    pieces = []
    known = []
    copies = jnp.broadcast_to(given[0][None], (lines, half, LANES))
    inverse = fetch(0)
    for i in range(sections):
        gathered = exchange(copies)
        if i + 1 == sections:
            stacked = apply_last(gathered, inverse, pieces)
            break
        piece, copies = apply(i, gathered, inverse)
        pieces.append(piece)
        gathered = exchange(copies)
        base, matrix, inverse = earlier(i + 1, given[i + 1], known)
        copies, parts = residual(i + 1, gathered, base, matrix)
        known.append(parts)

    found = lax.all_to_all(stacked, "sec", 0, 0, tiled=True)
    out = pl.pallas_call(
        unpack_kernel,
        out_shape=jax.ShapeDtypeStruct(right_side.shape[1:], f32),
        in_specs=[VMEM],
        out_specs=VMEM,
        compiler_params=params,
        name="unpack",
    )(found)
    return out[None]


def solution(mesh):
    return jax.shard_map(
        shards,
        mesh=mesh,
        in_specs=(P(None, "row", "sec"), P("sec", "row", None), P("sec", "row", None)),
        out_specs=P("sec", "row", None),
        check_vma=False,
    )
```

```python
import functools

import jax
import jax.numpy as jnp
from jax import lax
from jax.experimental import pallas as pl
from jax.experimental.pallas import tpu as pltpu
from jax.sharding import PartitionSpec as P

LANES = 128
VMEM = pl.BlockSpec(memory_space=pltpu.VMEM)
HBM = pl.BlockSpec(memory_space=pltpu.HBM)


def low_lanes(shape):
    return lax.broadcasted_iota(jnp.int32, shape, 1) < LANES // 2


def pack_kernel(rhs_ref, out_ref):
    groups, half, _ = out_ref.shape
    rows = rhs_ref[...]
    turned = jnp.concatenate([rows, rows], axis=0).T
    low = low_lanes((half, LANES))
    for group in range(groups):
        start = 2 * group * half
        top = turned[start : start + half]
        bottom = turned[start + half : start + 2 * half]
        out_ref[group] = jnp.where(low, top, bottom)


def unpack_kernel(packed_ref, out_ref):
    groups = packed_ref.shape[0]
    pieces = []
    for group in range(groups):
        tile = packed_ref[group]
        pieces += [tile, pltpu.roll(tile, LANES // 2, 1)]
    turned = jnp.concatenate(pieces, axis=0).T
    out_ref[...] = turned[: LANES // 2]


def split(values):
    high = values.astype(jnp.bfloat16)
    low = (values - high.astype(jnp.float32)).astype(jnp.bfloat16)
    return high, low


def spread(gathered_ref, whole_ref, parts_ref):
    devices, half, _ = gathered_ref.shape
    low = low_lanes((half, LANES))
    for pair in range(devices // 2):
        first = gathered_ref[2 * pair]
        second = gathered_ref[2 * pair + 1]
        lanes = slice(pair * LANES, (pair + 1) * LANES)
        whole_ref[:half, lanes] = jnp.where(low, first, pltpu.roll(second, LANES // 2, 1))
        whole_ref[half:, lanes] = jnp.where(low, pltpu.roll(first, LANES // 2, 1), second)
    high, rest = split(whole_ref[...])
    parts_ref[: 2 * half] = high
    parts_ref[2 * half :] = rest


def times(parts, matrix):
    cols = parts.shape[0] // 2
    high, low = split(matrix)
    dims = (((1,), (1,)), ((), ()))
    both = lax.dot_general(parts, high, dims, preferred_element_type=jnp.float32)
    rest = lax.dot_general(parts[:cols], low, dims, preferred_element_type=jnp.float32)
    return both[:cols] + (both[cols:] + rest)


def packed(turned):
    half = turned.shape[0] // 2
    return jnp.concatenate([turned[:half], turned[half:]], axis=1)


def fetch_kernel(index, matrix_ref, out_ref, sem):
    copy = pltpu.make_async_copy(matrix_ref.at[index], out_ref, sem)
    copy.start()
    copy.wait()


def apply_kernel(gathered_ref, matrix_ref, tile_ref, copies_ref, whole, parts):
    spread(gathered_ref, whole, parts)
    tile = packed(times(parts[...], matrix_ref[...]))
    tile_ref[...] = tile
    copies_ref[...] = jnp.broadcast_to(tile[None], copies_ref.shape)


def last_kernel(gathered_ref, matrix_ref, *refs):
    earlier_refs = refs[:-3]
    out_ref, whole, parts = refs[-3:]
    for i, piece_ref in enumerate(earlier_refs):
        out_ref[i] = piece_ref[...]
    spread(gathered_ref, whole, parts)
    out_ref[len(earlier_refs)] = packed(times(parts[...], matrix_ref[...]))


def residual_kernel(gathered_ref, base_ref, matrix_ref, copies_ref, parts, whole):
    spread(gathered_ref, whole, parts)
    tile = base_ref[...] - packed(times(parts[...], matrix_ref[...]))
    copies_ref[...] = jnp.broadcast_to(tile[None], copies_ref.shape)


def earlier_kernel(places, arrays, follow, *refs):
    count = len(places)
    base_ref = refs[0]
    panels = refs[1 : 1 + arrays]
    parts_refs = refs[1 + arrays : arrays + count]
    base_out, matrix_out, inverse_out, blocks, sems = refs[arrays + count :]
    targets = [blocks.at[k] for k in range(count - 1)] + [matrix_out]
    copies = []
    for k, (panel, slot) in enumerate(places):
        copies.append(pltpu.make_async_copy(panels[panel].at[slot], targets[k], sems.at[k]))
    copies.append(pltpu.make_async_copy(panels[0].at[follow], inverse_out, sems.at[count]))
    for copy in copies:
        copy.start()
    total = base_ref[...]
    for k in range(count - 1):
        copies[k].wait()
        total = total - packed(times(parts_refs[k][...], blocks[k]))
    base_out[...] = total
    copies[count - 1].wait()
    copies[count].wait()


def in_vmem(value):
    return pltpu.with_memory_space_constraint(value, pltpu.VMEM)


def in_hbm(value):
    return pltpu.with_memory_space_constraint(value, pltpu.HBM)


def shards(factor, inverse_blocks, right_side):
    sections = lax.axis_size("sec")
    segment = lax.axis_index("sec")
    lines = lax.axis_size("row")
    local_rows, block = factor.shape[1:]
    cols = right_side.shape[2] // sections
    half = cols // 2
    f32 = jnp.float32
    tile_in_vmem = pltpu.VMEM((half, LANES), f32)
    copies_in_vmem = pltpu.VMEM((lines, half, LANES), f32)
    parts_in_vmem = pltpu.VMEM((2 * cols, block), jnp.bfloat16)
    matrix_in_vmem = pltpu.VMEM((local_rows, block), f32)
    whole_scratch = pltpu.VMEM((cols, block), f32)
    params = pltpu.CompilerParams(vmem_limit_bytes=24 << 20)

    chunks = pl.pallas_call(
        pack_kernel,
        out_shape=jax.ShapeDtypeStruct((sections, half, LANES), f32),
        in_specs=[VMEM],
        out_specs=VMEM,
        compiler_params=params,
        name="pack",
    )(right_side[0])
    given = lax.all_to_all(chunks, "sec", 0, 0, tiled=True)

    def diagonal(factor, d):
        return lax.dynamic_index_in_dim(factor, jnp.minimum(segment + d, sections - 1), 0, False)

    first = lax.all_gather(jnp.stack([inverse_blocks[0], diagonal(factor, 1)]), "sec", axis=0)
    panels = {1: (first, 1)}
    given, factor = lax.optimization_barrier((given, factor))
    for group in ((2,), (3,), (4, 5), (6, 7)):
        sent = jnp.stack([diagonal(factor, d) for d in group])
        gathered = lax.all_gather(sent, "sec", axis=0)
        panels |= {d: (gathered, line) for line, d in enumerate(group)}

    def exchange(copies):
        return lax.all_to_all(copies, "row", 0, 0, tiled=True)

    def fetch(i):
        return pl.pallas_call(
            functools.partial(fetch_kernel, (i, 0)),
            out_shape=matrix_in_vmem,
            in_specs=[HBM],
            out_specs=VMEM,
            scratch_shapes=[pltpu.SemaphoreType.DMA],
            compiler_params=params,
            name=f"fetch_{i}",
        )(in_hbm(first))

    def apply(i, gathered, inverse):
        return pl.pallas_call(
            apply_kernel,
            out_shape=(tile_in_vmem, copies_in_vmem),
            in_specs=[VMEM, VMEM],
            out_specs=(VMEM, VMEM),
            scratch_shapes=[whole_scratch, parts_in_vmem],
            compiler_params=params,
            name=f"apply_{i}",
        )(in_vmem(gathered), in_vmem(inverse))

    def apply_last(gathered, inverse, pieces):
        return pl.pallas_call(
            last_kernel,
            out_shape=pltpu.VMEM((sections, half, LANES), f32),
            in_specs=[VMEM, VMEM] + [VMEM] * len(pieces),
            out_specs=VMEM,
            scratch_shapes=[whole_scratch, parts_in_vmem],
            compiler_params=params,
            name="apply_last",
        )(in_vmem(gathered), in_vmem(inverse), *[in_vmem(piece) for piece in pieces])

    def residual(j, gathered, base, matrix):
        return pl.pallas_call(
            residual_kernel,
            out_shape=(copies_in_vmem, parts_in_vmem),
            in_specs=[VMEM, VMEM, VMEM],
            out_specs=(VMEM, VMEM),
            scratch_shapes=[whole_scratch],
            compiler_params=params,
            name=f"residual_{j}",
        )(in_vmem(gathered), in_vmem(base), in_vmem(matrix))

    def earlier(j, base, known):
        arrays = [first]
        places = []
        for k in range(j):
            array, line = panels[j - k]
            if not any(array is other for other in arrays):
                arrays.append(array)
            index = [array is other for other in arrays].index(True)
            places.append((index, (k, line)))
        return pl.pallas_call(
            functools.partial(earlier_kernel, places, len(arrays), (j, 0)),
            out_shape=(tile_in_vmem, matrix_in_vmem, matrix_in_vmem),
            in_specs=[VMEM] + [HBM] * len(arrays) + [VMEM] * len(known),
            out_specs=(VMEM, VMEM, VMEM),
            scratch_shapes=[
                pltpu.VMEM((max(j - 1, 1), local_rows, block), f32),
                pltpu.SemaphoreType.DMA((j + 1,)),
            ],
            compiler_params=params,
            name=f"earlier_{j}",
        )(base, *[in_hbm(array) for array in arrays], *[in_vmem(parts) for parts in known])

    pieces = []
    known = []
    copies = jnp.broadcast_to(given[0][None], (lines, half, LANES))
    inverse = fetch(0)
    for i in range(sections):
        gathered = exchange(copies)
        if i + 1 == sections:
            stacked = apply_last(gathered, inverse, pieces)
            break
        piece, copies = apply(i, gathered, inverse)
        pieces.append(piece)
        gathered = exchange(copies)
        base, matrix, inverse = earlier(i + 1, given[i + 1], known)
        copies, parts = residual(i + 1, gathered, base, matrix)
        known.append(parts)

    found = lax.all_to_all(stacked, "sec", 0, 0, tiled=True)
    out = pl.pallas_call(
        unpack_kernel,
        out_shape=jax.ShapeDtypeStruct(right_side.shape[1:], f32),
        in_specs=[VMEM],
        out_specs=VMEM,
        compiler_params=params,
        name="unpack",
    )(found)
    return out[None]


def solution(mesh):
    return jax.shard_map(
        shards,
        mesh=mesh,
        in_specs=(P(None, "row", "sec"), P("sec", "row", None), P("sec", "row", None)),
        out_specs=P("sec", "row", None),
        check_vma=False,
    )
```
